32 devices in a mesh: groups: 2 (over x), blk: 8 (over z, y), rep: 2 (over core).
Axes of the slice: x: 2, y: 2, z: 4, core: 2. Of those that a mesh axis runs over, the one named last changes fastest.
Arguments:
- resident: bfloat16 [32768, 768], P(('groups', 'blk', 'rep')), parts along dimension 0, may hold values from -600 to 600
- ingest: bfloat16 [16384, 768], P(('groups', 'blk', 'rep')), parts along dimension 0, may hold values from -600 to 600
- cluster_ids: int32 [16384], P(('groups', 'blk', 'rep')), parts along dimension 0, may hold values from 0 to 127, as said below
Outputs:
- resident_score: float32 [32768], P(('groups', 'blk', 'rep')), parts along dimension 0
- ingest_score: float32 [16384], P(('groups', 'blk', 'rep')), parts along dimension 0
The draws below stay inside these ranges and needn't reach their ends.
There are 2 independent parts, one for each index of `groups`. The reference program is written for one: setup_inputs(seed, part) draws one part's arguments, and reference() takes and returns one part's arrays. A program takes and returns all parts, laid end to end along the dimension named above; each array names one. Nothing has to cross between parts.
Inputs may be any that keep to these rules, and one draw needn't show every extreme that they name: `cluster_ids`: clusters 16 * p to 16 * p + 15 belong to cycle position p. At most 96 documents of one device belong to one cycle position, and in every draw some cycle position receives 96 from every device.
All inputs are finite; a program needn't handle non-finite values.
Results may differ from the reference program's by a relative error of at most 0.0003.
Values may be sent and summed in bfloat16 or wider, within the bound.
No kernel may reach another device: no remote copies, remote signals or barrier semaphores. Data moves between devices by JAX's collectives and lax.ppermute only.
A program may use at most 64 MiB of HBM per device.

```python
import jax
import jax.numpy as jnp
from jax import lax

D = 768
INGEST_DEV = 512
CL_OWN = 16
CYCLE_STEPS = 4
CAP = 96
VISIT = 1536
RES_POS = 2048
RESIDENT = 16384
INGEST = 8192
CLUSTERS = 128
N_BLK = 8
N_REP = 2


def slot_layout(key):
    base = jax.random.fold_in(key, 7)
    sources = N_BLK * N_REP
    slot_total = N_BLK * CAP
    weights = jax.random.randint(jax.random.fold_in(base, 1), (N_BLK,), 1, 9)
    heavy = jax.random.randint(jax.random.fold_in(base, 2), (), 0, N_BLK)
    raw = jax.random.randint(jax.random.fold_in(base, 3), (sources, N_BLK, CAP), 0, 1024) * weights[None, :, None]
    owner_grid = jnp.arange(N_BLK, dtype=jnp.int32)[None, :, None]
    raw = raw + jnp.where(owner_grid == heavy, 16384, 0)
    ordering = jnp.arange(slot_total, dtype=jnp.int32).reshape(1, N_BLK, CAP)
    scores = (raw * slot_total + ordering).reshape(sources, slot_total)
    chosen = lax.top_k(scores, INGEST_DEV)[1]
    shuffle_bits = jax.random.randint(jax.random.fold_in(base, 4), (sources, INGEST_DEV), 0, 2 ** 20)
    shuffle_keys = shuffle_bits * INGEST_DEV + jnp.arange(INGEST_DEV, dtype=jnp.int32)[None, :]
    shuffled = jnp.take_along_axis(chosen, jnp.argsort(shuffle_keys, axis=1), axis=1)
    owners = shuffled // CAP
    within = jax.random.randint(jax.random.fold_in(base, 5), (sources, INGEST_DEV), 0, CL_OWN)
    return (owners * CL_OWN + within).reshape(-1).astype(jnp.int32)


def centroid_table(key):
    base = jax.random.fold_in(key, 101)
    span = 6 * CL_OWN
    basis = jax.random.truncated_normal(jax.random.fold_in(base, 1), -5.0, 5.0, (CLUSTERS, D), jnp.float32)
    indices = jnp.arange(CLUSTERS, dtype=jnp.int32)
    band = ((indices[None, :] - indices[:, None]) % CLUSTERS < span).astype(jnp.float32)
    centres = jnp.dot(band, basis, precision=lax.Precision.HIGHEST) / jnp.sqrt(jnp.float32(min(span, CLUSTERS)))
    spread = jnp.exp(jax.random.uniform(jax.random.fold_in(base, 2), (CLUSTERS,), jnp.float32, jnp.log(0.4), jnp.log(2.0)))
    return (centres, spread)


def embed_rows(key, clusters, salt):
    centres, spread = centroid_table(key)
    salted = jax.random.fold_in(key, salt)
    count = clusters.shape[0]
    jitter = jax.random.truncated_normal(jax.random.fold_in(salted, 1), -5.0, 5.0, (count, D), jnp.float32)
    scales = jnp.exp(jax.random.uniform(jax.random.fold_in(salted, 2), (count,), jnp.float32, 0.0, jnp.log(10.0)))
    rows = (0.5 * centres[clusters] + spread[clusters][:, None] * jitter) * scales[:, None]
    return rows.astype(jnp.bfloat16)


def draw_resident(key, part):
    positions = jnp.arange(RESIDENT, dtype=jnp.int32) // RES_POS
    within = jax.random.randint(jax.random.fold_in(key, 201), (RESIDENT,), 0, CL_OWN)
    return embed_rows(key, positions * CL_OWN + within, 202)


def draw_ingest(key, part):
    clusters = slot_layout(key)
    rows = embed_rows(key, clusters, 203).astype(jnp.float32)
    resident_rows = draw_resident(key, part).astype(jnp.float32)
    base = jax.random.fold_in(key, 301)
    owners = clusters // CL_OWN
    offsets = jax.random.randint(jax.random.fold_in(base, 1), (INGEST,), 1, CYCLE_STEPS + 1)
    picks = jax.random.randint(jax.random.fold_in(base, 2), (INGEST,), 0, RES_POS)
    sources = (owners + offsets) % N_BLK * RES_POS + picks
    copied = resident_rows[sources]
    level = jnp.sqrt(jnp.mean(copied * copied, axis=1) + 1e-12)
    noise = jax.random.truncated_normal(jax.random.fold_in(base, 3), -3.0, 3.0, (INGEST, D), jnp.float32)
    factor = jax.random.uniform(jax.random.fold_in(base, 4), (INGEST,), jnp.float32, 0.5, 1.0)
    near = (copied + 0.02 * level[:, None] * noise) * factor[:, None]
    planted = jax.random.randint(jax.random.fold_in(base, 5), (INGEST,), 0, 4) == 0
    rows = jnp.where(planted[:, None], near, rows)
    return rows.astype(jnp.bfloat16)


def draw_cluster_ids(key, part):
    return slot_layout(key)


def setup_inputs(seed: int = 0, part: int = 0) -> dict:
    splits = jax.random.split(jax.random.key(seed), 4)
    part_keys = jax.random.split(jax.random.fold_in(splits[3], part), 4)
    resident = draw_resident(jax.random.fold_in(jax.random.fold_in(splits[3], part), 71), part)
    ingest = draw_ingest(jax.random.fold_in(jax.random.fold_in(splits[3], part), 71), part)
    cluster_ids = draw_cluster_ids(jax.random.fold_in(jax.random.fold_in(splits[3], part), 71), part)
    return {"resident": resident, "ingest": ingest, "cluster_ids": cluster_ids}


temper = 0.2
epsilon = 1e-06

def unit_rows(rows):
    values = rows.astype(jnp.float32)
    squares = lax.optimization_barrier(jnp.sum(values * values, axis=-1, keepdims=True)) + epsilon
    factor = lax.rsqrt(squares)
    return (values * factor).astype(jnp.bfloat16)

def reference(resident, ingest, cluster_ids):
    unit_resident = unit_rows(resident).reshape(N_BLK, RES_POS, D)
    unit_ingest = unit_rows(ingest)
    owners = cluster_ids // CL_OWN
    sources = N_BLK * N_REP
    grouped = owners.reshape(sources, INGEST_DEV)
    onehot = (grouped[:, :, None] == jnp.arange(N_BLK, dtype=jnp.int32)[None, None, :]).astype(jnp.int32)
    rank_within = lax.optimization_barrier(jnp.sum((jnp.cumsum(onehot, axis=1) - onehot) * onehot, axis=2))
    source_ids = jnp.arange(sources, dtype=jnp.int32)[:, None]
    slot_index = (source_ids % N_REP * (N_BLK * CAP) + source_ids // N_REP * CAP + rank_within).reshape(INGEST)
    visiting = jnp.zeros((N_BLK, VISIT, D), jnp.bfloat16).at[owners, slot_index].set(unit_ingest)
    occupied = jnp.zeros((N_BLK, VISIT), jnp.float32).at[owners, slot_index].set(1.0)

    def per_owner(pieces):
        position, visitors, occupancy = pieces
        visit_sum = jnp.zeros((VISIT,), jnp.float32)
        partials = []
        for offset in range(CYCLE_STEPS + 1):
            resident_block = lax.dynamic_index_in_dim(unit_resident, (position + offset) % N_BLK, 0, keepdims=False)
            scores = jnp.dot(visitors, resident_block.T, preferred_element_type=jnp.float32)
            kernel = jnp.exp((scores - 1.0) / temper)
            visit_sum = visit_sum + lax.optimization_barrier(jnp.sum(kernel, axis=1))
            partials.append(lax.optimization_barrier(jnp.sum(kernel * occupancy[:, None], axis=0)))
        return (visit_sum, jnp.stack(partials))
    visit_sums, resident_parts = lax.map(per_owner, (jnp.arange(N_BLK, dtype=jnp.int32), visiting, occupied))
    resident_density = resident_parts[:, 0]
    for offset in range(1, CYCLE_STEPS + 1):
        resident_density = resident_density + jnp.roll(resident_parts[:, offset], offset, axis=0)
    ingest_density = visit_sums[owners, slot_index]
    return (jnp.log1p(resident_density.reshape(RESIDENT)), jnp.log1p(ingest_density))
```

```python
import functools

import jax
import jax.numpy as jnp
from jax import lax
from jax.experimental import pallas as pl
from jax.experimental.pallas import tpu as pltpu
from jax.sharding import PartitionSpec as P

CL_OWN = 16
CYCLE_STEPS = 4
INGEST_DEV = 512

temper = 0.2
epsilon = 1e-06


GAIN = 1.4426950408889634 / temper
OFF = -1e30
LANES = 128
NT = (((1,), (1,)), ((), ()))
VMEM = pl.BlockSpec(memory_space=pltpu.VMEM)
SMEM = pl.BlockSpec(memory_space=pltpu.SMEM)


def unit_body(count, x_ref, *o_refs):
    rows = x_ref.shape[0] // count
    for k in range(count):
        values = x_ref[k * rows : (k + 1) * rows, :].astype(jnp.float32)
        squares = jnp.sum(values * values, axis=-1, keepdims=True) + epsilon
        o_refs[k][...] = (values * lax.rsqrt(squares)).astype(jnp.bfloat16)


def unit_block(rows, first, size, count, name):
    columns = rows.shape[1]
    piece = jax.ShapeDtypeStruct((size // count, columns), jnp.bfloat16)
    out = pl.pallas_call(
        functools.partial(unit_body, count),
        grid=(1,),
        in_specs=[pl.BlockSpec((size, columns), lambda g: (first, 0))],
        out_specs=[pl.BlockSpec((size // count, columns), lambda g: (0, 0))] * count,
        out_shape=[piece] * count,
        name=name,
        cost_estimate=pl.CostEstimate(
            flops=size * columns * 300, bytes_accessed=size * columns * 4, transcendentals=size
        ),
    )(rows)
    return list(out)


def sums_body(n_docs, n_res, sides, doc_in, res_in, cycle, *refs):
    refs = list(refs)
    place_ref = refs.pop(0)
    docs = [refs.pop(0) for _ in range(n_docs)]
    owners = [refs.pop(0) for _ in range(n_docs)]
    res = [refs.pop(0) for _ in range(n_res)]
    doc_prev = [refs.pop(0) if f else None for f in doc_in]
    res_prev = [refs.pop(0) if f else None for f in res_in]
    doc_out = [refs.pop(0) for _ in range(n_docs)]
    res_out = [refs.pop(0) for _ in range(n_res)]
    first_res = [True] * n_res
    for i in range(n_docs):
        n = docs[i].shape[0]
        doc = docs[i][...]
        bias = {}
        for side in sorted(set(sides)):
            ahead = place_ref[side] - owners[i][...]
            ahead = jnp.where(ahead < 0, ahead + cycle, ahead)
            row = jnp.where(ahead <= CYCLE_STEPS, -GAIN, OFF).astype(jnp.float32)
            bias[side] = jnp.broadcast_to(row, (LANES, n)).T
        tile = 512
        work = [(j, t) for j in range(n_res) for t in range(res[j].shape[0] // tile)]

        def scores(j, t):
            return lax.dot_general(
                doc, res[j][t * tile : (t + 1) * tile, :], NT, preferred_element_type=jnp.float32
            )

        total = jnp.zeros((n, LANES), jnp.float32)
        ahead_s = scores(*work[0])
        for w, (j, t) in enumerate(work):
            s = ahead_s
            if w + 1 < len(work):
                ahead_s = scores(*work[w + 1])
            for q in range(tile // LANES):
                k = jnp.exp2(s[:, q * LANES : (q + 1) * LANES] * GAIN + bias[sides[j]])
                total = total + k
                col = slice(t * tile + q * LANES, t * tile + (q + 1) * LANES)
                part = jnp.sum(k, axis=0, keepdims=True)
                if first_res[j]:
                    if res_prev[j] is not None:
                        part = part + res_prev[j][:, col]
                    res_out[j][:, col] = part
                else:
                    res_out[j][:, col] = res_out[j][:, col] + part
        for j in range(n_res):
            first_res[j] = False
        row = jnp.sum(total.T, axis=0, keepdims=True)
        if doc_prev[i] is not None:
            row = row + doc_prev[i][...]
        doc_out[i][...] = row


def kernel_sums(name, cycle, place, docs, owners, res, sides, doc_prev, res_prev):
    doc_in = tuple(x is not None for x in doc_prev)
    res_in = tuple(x is not None for x in res_prev)
    n = sum(x.shape[0] for x in docs)
    m = sum(x.shape[0] for x in res)
    operands = [place, *docs, *owners, *res]
    operands += [x for x in doc_prev if x is not None]
    operands += [x for x in res_prev if x is not None]
    out = pl.pallas_call(
        functools.partial(sums_body, len(docs), len(res), tuple(sides), doc_in, res_in, cycle),
        in_specs=[SMEM] + [VMEM] * (len(operands) - 1),
        out_specs=[VMEM] * (len(docs) + len(res)),
        out_shape=[jax.ShapeDtypeStruct((1, x.shape[0]), jnp.float32) for x in (*docs, *res)],
        name=name,
        compiler_params=pltpu.CompilerParams(vmem_limit_bytes=24 * 2**20),
        cost_estimate=pl.CostEstimate(
            flops=2 * n * m * docs[0].shape[1], bytes_accessed=(n + m) * 1536, transcendentals=n * m
        ),
    )(*operands)
    return list(out[: len(docs)]), list(out[len(docs) :])


def line_order(count):
    return list(range(0, count, 2)) + list(reversed(range(1, count, 2)))


def dense(resident, ingest, cluster_ids):
    cycle = lax.axis_size("blk")
    lines = cycle // 2
    order = line_order(lines)
    half = ingest.shape[0] // 2

    def along(value, steps):
        pairs = [
            (order[k] * 2 + y, order[(k + steps) % lines] * 2 + y) for k in range(lines) for y in range(2)
        ]
        return lax.ppermute(value, "blk", pairs)

    def mate(value):
        return lax.ppermute(value, "blk", [(p, p ^ 1) for p in range(cycle)])

    def twin(value):
        return lax.ppermute(value, "rep", [(0, 1), (1, 0)])

    here = lax.axis_index("blk")
    place = jnp.stack([here, here ^ 1]).astype(jnp.int32)
    owner = (cluster_ids // CL_OWN).reshape(1, -1)

    own = [unit_block(ingest, k, half, 1, "unit_ingest_%d" % k)[0] for k in range(2)]
    chunks = [own]
    for _ in range(1, lines):
        chunks.append([along(x, 1) for x in chunks[-1]])
    owners = [owner] + [along(owner, d) for d in range(1, lines)]
    owners = [[x[:, :half], x[:, half:]] for x in owners]

    r0 = unit_block(resident, 0, resident.shape[0], 2, "unit_resident")
    r2 = [mate(x) for x in r0]
    r1 = [twin(x) for x in r0]
    r3 = [twin(x) for x in r2]

    near = [0, 0, 0, 0]
    sums = functools.partial(kernel_sums, cycle=cycle, place=place)

    none2, none4 = [None] * 2, [None] * 4
    d_own, a0 = sums("own_r0", docs=chunks[0], owners=owners[0], res=r0, sides=[0, 0], doc_prev=none2, res_prev=none2)
    d_own, a1 = sums("own_r1", docs=chunks[0], owners=owners[0], res=r1, sides=[0, 0], doc_prev=d_own, res_prev=none2)
    a01 = a0 + a1
    r01 = r0 + r1
    d1 = []
    for k in range(2):
        d, a01 = sums(
            "z1_%d" % k, docs=[chunks[1][k]], owners=[owners[1][k]], res=r01, sides=near, doc_prev=[None], res_prev=a01
        )
        d1 += d
    ra = [r2[0], r3[0]]
    rb = [r2[1], r3[1]]
    d, aa = sums(
        "mate_a", docs=chunks[0] + chunks[1], owners=owners[0] + owners[1], res=ra, sides=[1, 1],
        doc_prev=d_own + d1, res_prev=none2,
    )
    d_own, d1 = d[:2], d[2:]
    d2 = []
    d, a = sums(
        "z2_0", docs=[chunks[2][0]], owners=[owners[2][0]], res=r01 + ra, sides=[0, 0, 0, 0, 1, 1],
        doc_prev=[None], res_prev=a01 + aa,
    )
    d2 += d
    a01, aa = a[:4], a[4:]
    d, ab = sums(
        "mate_b", docs=chunks[0] + chunks[1] + chunks[2][:1], owners=owners[0] + owners[1] + owners[2][:1],
        res=rb, sides=[1, 1], doc_prev=d_own + d1 + d2, res_prev=none2,
    )
    d_own, d1, d2 = d[:2], d[2:4], d[4:]
    every = r01 + ra + rb
    d, a = sums(
        "z2_1", docs=[chunks[2][1]], owners=[owners[2][1]], res=every, sides=near + [1] * 4,
        doc_prev=[None], res_prev=a01 + aa + ab,
    )
    d2 += d
    d3a, a = sums(
        "z3_0", docs=[chunks[3][0]], owners=[owners[3][0]], res=every, sides=near + [1] * 4,
        doc_prev=[None], res_prev=a,
    )
    d3b, am = sums(
        "z3_1m", docs=[chunks[3][1]], owners=[owners[3][1]], res=ra + rb, sides=[1] * 4,
        doc_prev=[None], res_prev=a[4:],
    )
    to_mate = jnp.concatenate([am[0], am[2], am[1], am[3]], axis=1)
    from_mate = mate(to_mate)
    d3b, an = sums(
        "z3_1n", docs=[chunks[3][1]], owners=[owners[3][1]], res=r01, sides=near,
        doc_prev=d3b, res_prev=a[:4],
    )
    rows = resident.shape[0]
    back = twin(jnp.concatenate(an[2:], axis=1) + from_mate[:, rows:])
    resident_density = jnp.concatenate(an[:2], axis=1) + from_mate[:, :rows] + back

    ingest_density = jnp.concatenate(d_own, axis=1)
    for d, parts in ((1, d1), (2, d2), (3, d3a + d3b)):
        ingest_density = ingest_density + along(jnp.concatenate(parts, axis=1), -d)
    return (jnp.log1p(resident_density).reshape(-1), jnp.log1p(ingest_density).reshape(-1))


def shifted(value, axis, steps):
    count = lax.axis_size(axis)
    pairs = [(source, (source + steps) % count) for source in range(count)]
    return lax.ppermute(value, axis, pairs)


def unit_rows(rows):
    values = rows.astype(jnp.float32)
    squares = jnp.sum(values * values, axis=-1, keepdims=True) + epsilon
    factor = lax.rsqrt(squares)
    return (values * factor).astype(jnp.bfloat16)


def scanned_sums(visitors, occupancy, residents):
    count_rows = visitors.shape[0]
    block_rows = 512
    num_blocks = count_rows // block_rows
    visit_blocks = visitors.reshape(num_blocks, block_rows, visitors.shape[1])
    live_blocks = occupancy.astype(jnp.float32).reshape(num_blocks, block_rows)

    def tile_sums(running, pieces):
        visit_tile, live_tile = pieces
        scores = jnp.einsum("vd,rd->vr", visit_tile, residents, preferred_element_type=jnp.float32)
        kernel = jnp.exp((scores - 1.0) / temper)
        return (running + jnp.sum(kernel * live_tile[:, None], axis=0), jnp.sum(kernel, axis=1))

    resident_part, visit_parts = lax.scan(
        tile_sums, jnp.zeros((residents.shape[0],), jnp.float32), (visit_blocks, live_blocks)
    )
    return (visit_parts.reshape(count_rows), resident_part)


def cyclic(resident, ingest, cluster_ids):
    cycle_size = lax.axis_size("blk")
    slot_count = 3 * INGEST_DEV // (2 * cycle_size)
    columns = ingest.shape[1]
    owners = cluster_ids // CL_OWN
    onehot = (owners[:, None] == jnp.arange(cycle_size, dtype=jnp.int32)[None, :]).astype(jnp.int32)
    rank_within = jnp.sum((jnp.cumsum(onehot, axis=0) - onehot) * onehot, axis=1)
    targets = owners * slot_count + rank_within
    unit_ingest = unit_rows(ingest)
    outgoing = jnp.zeros((cycle_size * slot_count, columns), jnp.bfloat16).at[targets].set(unit_ingest)
    filled = (
        jnp.zeros((cycle_size * slot_count,), jnp.bfloat16)
        .at[targets]
        .set(jnp.ones((ingest.shape[0],), jnp.bfloat16))
    )
    exchange = functools.partial(lax.all_to_all, axis_name="blk", split_axis=0, concat_axis=0, tiled=True)
    arrived = exchange(outgoing.reshape(cycle_size, slot_count, columns))
    present = exchange(filled.reshape(cycle_size, slot_count))
    visitors = lax.all_gather(arrived.reshape(cycle_size * slot_count, columns), "rep", axis=0, tiled=True)
    marked = lax.all_gather(present.reshape(cycle_size * slot_count), "rep", axis=0, tiled=True)
    visit_total = jnp.zeros((visitors.shape[0],), jnp.float32)
    resident_total = jnp.zeros((resident.shape[0],), jnp.float32)
    moving = unit_rows(resident)
    for rotation in range(CYCLE_STEPS + 1):
        if rotation > 0:
            moving = shifted(moving, "blk", -1)
            resident_total = shifted(resident_total, "blk", -1)
        visit_part, resident_part = scanned_sums(visitors, marked, moving)
        visit_total = visit_total + visit_part
        resident_total = resident_total + resident_part
    resident_total = shifted(resident_total, "blk", CYCLE_STEPS)
    own_sums = lax.psum_scatter(visit_total, "rep", scatter_dimension=0, tiled=True)
    returned = exchange(own_sums.reshape(cycle_size, slot_count))
    density = returned.reshape(cycle_size * slot_count)[targets]
    return (jnp.log1p(resident_total), jnp.log1p(density))


def solution(mesh):
    spread = ("groups", "blk", "rep")
    in_specs = (P(spread, None), P(spread, None), P(spread))
    out_specs = (P(spread), P(spread))
    short = mesh.shape["blk"] == 8 and mesh.shape["rep"] == 2
    return jax.shard_map(
        dense if short else cyclic, mesh=mesh, in_specs=in_specs, out_specs=out_specs, check_vma=False
    )
```

```python
import functools

import jax
import jax.numpy as jnp
from jax import lax
from jax.experimental import pallas as pl
from jax.experimental.pallas import tpu as pltpu
from jax.sharding import PartitionSpec as P


CL_OWN = 16
CYCLE_STEPS = 4
INGEST_DEV = 512

temper = 0.2
epsilon = 1e-06


GAIN = 1.4426950408889634 / temper
OFF = -1e30
LANES = 128
NT = (((1,), (1,)), ((), ()))
VMEM = pl.BlockSpec(memory_space=pltpu.VMEM)
TILE = 512
FIRST = 8


def unit_body(parts, n_more, x_ref, *refs):
    for part, o_ref in zip(parts, refs[n_more:]):
        values = x_ref[part, :].astype(jnp.float32)
        squares = jnp.sum(values * values, axis=-1, keepdims=True) + epsilon
        o_ref[...] = (values * lax.rsqrt(squares)).astype(jnp.bfloat16)


def unit_rows_call(rows, parts, more):
    columns = rows.shape[1]
    sizes = [part.stop - part.start for part in parts]
    return pl.pallas_call(
        functools.partial(unit_body, parts, len(more)),
        in_specs=[VMEM] * (1 + len(more)),
        out_specs=[VMEM] * len(parts),
        out_shape=[pltpu.VMEM((size, columns), jnp.bfloat16) for size in sizes],
        compiler_params=pltpu.CompilerParams(vmem_limit_bytes=24 * 2**20),
        cost_estimate=pl.CostEstimate(
            flops=sum(sizes) * columns * 300, bytes_accessed=sum(sizes) * columns * 4, transcendentals=sum(sizes)
        ),
    )(rows, *more)


def sums_body(n_docs, n_res, cycle, cuts, sides, doc_in, res_in, *refs):
    refs = list(refs)
    place_ref = refs.pop(0)
    docs = [refs.pop(0) for _ in range(n_docs)]
    owners = [refs.pop(0) for _ in range(n_docs)]
    res = [refs.pop(0) for _ in range(n_res)]
    doc_prev = [refs.pop(0) if f else None for f in doc_in]
    res_prev = [refs.pop(0) if f else None for f in res_in]
    doc_out = [refs.pop(0) for _ in range(n_docs)]
    res_out = [refs.pop(0) for _ in range(n_res)]
    work = []
    for i in range(n_docs):
        for j in range(n_res):
            rows = res[j].shape[0]
            tile = min(TILE, rows)
            work += [(i, j, t, tile) for t in range(0, rows, tile)]

    def scores(i, j, t, tile):
        return lax.dot_general(
            docs[i][...], res[j][t : t + tile, :], NT, preferred_element_type=jnp.float32
        )

    seen = set()
    doing = None
    ahead = scores(*work[0])
    for w, (i, j, t, tile) in enumerate(work):
        n = docs[i].shape[0]
        if doing != i:
            doing = i
            bias = {}
            for side in sorted(set(sides)):
                steps = place_ref[side : side + 1, :n] - owners[i][:, cuts[i]]
                steps = jnp.where(steps < 0, steps + cycle, steps)
                row = jnp.where(steps <= CYCLE_STEPS, -GAIN, OFF).astype(jnp.float32)
                bias[side] = jnp.broadcast_to(row, (LANES, n)).T
            total = jnp.zeros((n, LANES), jnp.float32)
        s = ahead
        if w + 1 < len(work):
            ahead = scores(*work[w + 1])
        for q in range(0, tile, LANES):
            k = jnp.exp2(s[:, q : q + LANES] * GAIN + bias[sides[j]])
            total = total + k
            part = jnp.sum(k, axis=0, keepdims=True)
            col = slice(t + q, t + q + LANES)
            if (j, t + q) in seen:
                part = part + res_out[j][:, col]
            elif res_prev[j] is not None:
                part = part + res_prev[j][:, col]
            seen.add((j, t + q))
            res_out[j][:, col] = part
        if w + 1 == len(work) or work[w + 1][0] != i:
            row = jnp.sum(total.T, axis=0, keepdims=True)
            if doc_prev[i] is not None:
                row = row + doc_prev[i][...]
            doc_out[i][...] = row


def held(value):
    return pltpu.with_memory_space_constraint(value, pltpu.VMEM)


def kernel_sums(cycle, place, chunks, res, sides, doc_prev, res_prev):
    docs, owners, cuts = zip(*chunks)
    doc_in = tuple(x is not None for x in doc_prev)
    res_in = tuple(x is not None for x in res_prev)
    n = sum(x.shape[0] for x in docs)
    m = sum(x.shape[0] for x in res)
    docs = [held(x) for x in docs]
    res = [held(x) for x in res]
    operands = [place, *docs, *owners, *res]
    operands += [x for x in doc_prev if x is not None]
    operands += [x for x in res_prev if x is not None]
    out = pl.pallas_call(
        functools.partial(sums_body, len(docs), len(res), cycle, cuts, tuple(sides), doc_in, res_in),
        in_specs=[VMEM] * len(operands),
        out_specs=[VMEM] * (len(docs) + len(res)),
        out_shape=[jax.ShapeDtypeStruct((1, x.shape[0]), jnp.float32) for x in (*docs, *res)],
        compiler_params=pltpu.CompilerParams(vmem_limit_bytes=24 * 2**20),
        cost_estimate=pl.CostEstimate(
            flops=2 * n * m * docs[0].shape[1], bytes_accessed=(n + m) * 1536, transcendentals=n * m
        ),
    )(*operands)
    return list(out[: len(docs)]), list(out[len(docs) :])


def line_order(count):
    return list(range(0, count, 2)) + list(reversed(range(1, count, 2)))


def dense(resident, ingest, cluster_ids):
    return dense_body(resident, ingest, cluster_ids)


def dense_body(resident, ingest, cluster_ids):
    cycle = lax.axis_size("blk")
    lines = cycle // 2
    order = line_order(lines)
    count, _ = ingest.shape
    cuts = (0, count * FIRST // 16, count)
    parts = [slice(cuts[k], cuts[k + 1]) for k in range(2)]

    def along(value, steps):
        pairs = [
            (order[k] * 2 + y, order[(k + steps) % lines] * 2 + y) for k in range(lines) for y in range(2)
        ]
        return lax.ppermute(value, "blk", pairs)

    def mate(value):
        return lax.ppermute(value, "blk", [(p, p ^ 1) for p in range(cycle)])

    def twin(value):
        return lax.ppermute(value, "rep", [(0, 1), (1, 0)])

    here = lax.axis_index("blk")
    place = jnp.stack([here, here ^ 1]).astype(jnp.int32)
    place = jnp.broadcast_to(place[:, None], (2, count))

    own = [unit_rows_call(ingest, [parts[k]], [resident])[0] for k in range(2)]
    units = [own]
    owners = [(cluster_ids // CL_OWN).reshape(1, count)]
    for d in range(1, lines):
        units.append([along(units[-1][k], 1) for k in range(2)])
        owners.append(along(owners[-1], 1))
    chunks = [[(units[d][k], owners[d], parts[k]) for k in range(2)] for d in range(lines)]

    rows = resident.shape[0]
    whole = slice(0, rows)
    halves = [slice(0, rows // 2), slice(rows // 2, rows)]
    r0, *r0_halves = unit_rows_call(resident, [whole, *halves], [])
    r2 = [mate(r0_halves[k]) for k in range(2)]
    r1 = twin(r0)
    r3 = [twin(r2[k]) for k in range(2)]
    ra = [r2[0], r3[0]]
    rb = [r2[1], r3[1]]

    def sums(docs, res, sides, doc_prev, res_prev):
        return kernel_sums(cycle, place, docs, res, sides, doc_prev, res_prev)

    d_own, a0 = sums(chunks[0], [r0], [0], [None] * 2, [None])
    d_own, a1 = sums(chunks[0], [r1], [0], d_own, [None])
    a = a0 + a1
    d1, d2 = [], []
    for k in range(2):
        d, a = sums(chunks[1][k : k + 1], [r0, r1], [0, 0], [None], a)
        d1 += d
    d, aa = sums(chunks[0] + chunks[1], ra, [1, 1], d_own + d1, [None] * 2)
    d_own, d1 = d[:2], d[2:]
    a = a + aa
    for k in range(2):
        d, a = sums(chunks[2][k : k + 1], [r0, r1, *ra], [0, 0, 1, 1], [None], a)
        d2 += d
    d, ab = sums(chunks[0] + chunks[1] + chunks[2], rb, [1, 1], d_own + d1 + d2, [None] * 2)
    d_own, d1, d2 = d[:2], d[2:4], d[4:]
    d3a, a = sums(chunks[3][:1], [r0, r1, *ra, *rb], [0, 0, 1, 1, 1, 1], [None], a + ab)
    d3b, am = sums(chunks[3][1:], ra + rb, [1] * 4, [None], a[2:])
    to_mate = jnp.concatenate([am[0], am[2], am[1], am[3]], axis=1)
    from_mate = mate(to_mate)
    d3b, an = sums(chunks[3][1:], [r0, r1], [0, 0], d3b, a[:2])
    to_twin = an[1] + from_mate[:, rows:]
    from_twin = twin(to_twin)
    resident_density = an[0] + from_mate[:, :rows] + from_twin

    ingest_density = jnp.concatenate(d_own, axis=1)
    for d, pieces in ((1, d1), (2, d2), (3, d3a + d3b)):
        pieces = jnp.concatenate(pieces, axis=1)
        ingest_density = ingest_density + along(pieces, -d)
    return (jnp.log1p(resident_density).reshape(-1), jnp.log1p(ingest_density).reshape(-1))


def shifted(value, axis, steps):
    count = lax.axis_size(axis)
    pairs = [(source, (source + steps) % count) for source in range(count)]
    return lax.ppermute(value, axis, pairs)


def unit_rows(rows):
    values = rows.astype(jnp.float32)
    squares = jnp.sum(values * values, axis=-1, keepdims=True) + epsilon
    factor = lax.rsqrt(squares)
    return (values * factor).astype(jnp.bfloat16)


def scanned_sums(visitors, occupancy, residents):
    count_rows = visitors.shape[0]
    block_rows = 512
    num_blocks = count_rows // block_rows
    visit_blocks = visitors.reshape(num_blocks, block_rows, visitors.shape[1])
    live_blocks = occupancy.astype(jnp.float32).reshape(num_blocks, block_rows)

    def tile_sums(running, pieces):
        visit_tile, live_tile = pieces
        scores = jnp.einsum("vd,rd->vr", visit_tile, residents, preferred_element_type=jnp.float32)
        kernel = jnp.exp((scores - 1.0) / temper)
        return (running + jnp.sum(kernel * live_tile[:, None], axis=0), jnp.sum(kernel, axis=1))

    resident_part, visit_parts = lax.scan(
        tile_sums, jnp.zeros((residents.shape[0],), jnp.float32), (visit_blocks, live_blocks)
    )
    return (visit_parts.reshape(count_rows), resident_part)


def cyclic(resident, ingest, cluster_ids):
    cycle_size = lax.axis_size("blk")
    slot_count = 3 * INGEST_DEV // (2 * cycle_size)
    columns = ingest.shape[1]
    owners = cluster_ids // CL_OWN
    onehot = (owners[:, None] == jnp.arange(cycle_size, dtype=jnp.int32)[None, :]).astype(jnp.int32)
    rank_within = jnp.sum((jnp.cumsum(onehot, axis=0) - onehot) * onehot, axis=1)
    targets = owners * slot_count + rank_within
    unit_ingest = unit_rows(ingest)
    outgoing = jnp.zeros((cycle_size * slot_count, columns), jnp.bfloat16).at[targets].set(unit_ingest)
    filled = (
        jnp.zeros((cycle_size * slot_count,), jnp.bfloat16)
        .at[targets]
        .set(jnp.ones((ingest.shape[0],), jnp.bfloat16))
    )
    exchange = functools.partial(lax.all_to_all, axis_name="blk", split_axis=0, concat_axis=0, tiled=True)
    arrived = exchange(outgoing.reshape(cycle_size, slot_count, columns))
    present = exchange(filled.reshape(cycle_size, slot_count))
    visitors = lax.all_gather(arrived.reshape(cycle_size * slot_count, columns), "rep", axis=0, tiled=True)
    marked = lax.all_gather(present.reshape(cycle_size * slot_count), "rep", axis=0, tiled=True)
    visit_total = jnp.zeros((visitors.shape[0],), jnp.float32)
    resident_total = jnp.zeros((resident.shape[0],), jnp.float32)
    moving = unit_rows(resident)
    for rotation in range(CYCLE_STEPS + 1):
        if rotation > 0:
            moving = shifted(moving, "blk", -1)
            resident_total = shifted(resident_total, "blk", -1)
        visit_part, resident_part = scanned_sums(visitors, marked, moving)
        visit_total = visit_total + visit_part
        resident_total = resident_total + resident_part
    resident_total = shifted(resident_total, "blk", CYCLE_STEPS)
    own_sums = lax.psum_scatter(visit_total, "rep", scatter_dimension=0, tiled=True)
    returned = exchange(own_sums.reshape(cycle_size, slot_count))
    density = returned.reshape(cycle_size * slot_count)[targets]
    return (jnp.log1p(resident_total), jnp.log1p(density))


def solution(mesh):
    spread = ("groups", "blk", "rep")
    in_specs = (P(spread, None), P(spread, None), P(spread))
    out_specs = (P(spread), P(spread))
    short = mesh.shape["blk"] == 8 and mesh.shape["rep"] == 2
    return jax.shard_map(
        dense if short else cyclic, mesh=mesh, in_specs=in_specs, out_specs=out_specs, check_vma=False
    )
```

```python
import functools

import jax
import jax.numpy as jnp
from jax import lax
from jax.experimental import pallas as pl
from jax.experimental.pallas import tpu as pltpu
from jax.sharding import PartitionSpec as P


CL_OWN = 16
CYCLE_STEPS = 4
INGEST_DEV = 512

temper = 0.2
epsilon = 1e-06


GAIN = 1.4426950408889634 / temper
OFF = -1e30
LANES = 128
NT = (((1,), (1,)), ((), ()))
VMEM = pl.BlockSpec(memory_space=pltpu.VMEM)
TILE = 512
FIRST = 8


def unit(values):
    values = values.astype(jnp.float32)
    squares = jnp.sum(values * values, axis=-1, keepdims=True) + epsilon
    return (values * lax.rsqrt(squares)).astype(jnp.bfloat16)


def unit_body(pieces, outs, x_ref, *refs):
    o_refs, raw_ref, sem = refs[: len(outs)], refs[-2], refs[-1]
    copies = [
        pltpu.make_async_copy(x_ref.at[piece], raw_ref.at[piece], sem.at[k]) for k, piece in enumerate(pieces)
    ]
    for copy in copies:
        copy.start()
    for copy, piece in zip(copies, pieces):
        copy.wait()
        rows = unit(raw_ref[piece, :])
        for o_ref, out in zip(o_refs, outs):
            if out.start <= piece.start and piece.stop <= out.stop:
                o_ref[piece.start - out.start : piece.stop - out.start, :] = rows


def unit_rows_call(rows, pieces, outs):
    columns = rows.shape[1]
    sizes = [out.stop - out.start for out in outs]
    return list(
        pl.pallas_call(
            functools.partial(unit_body, pieces, outs),
            in_specs=[pl.BlockSpec(memory_space=pltpu.HBM)],
            out_specs=[VMEM] * len(outs),
            out_shape=[pltpu.VMEM((size, columns), jnp.bfloat16) for size in sizes],
            scratch_shapes=[pltpu.VMEM(rows.shape, jnp.bfloat16), pltpu.SemaphoreType.DMA((len(pieces),))],
            compiler_params=pltpu.CompilerParams(vmem_limit_bytes=24 * 2**20),
            cost_estimate=pl.CostEstimate(
                flops=rows.size * 300, bytes_accessed=rows.size * 4, transcendentals=rows.shape[0]
            ),
        )(pltpu.with_memory_space_constraint(rows, pltpu.HBM))
    )


def sums_body(n_docs, n_res, cycle, cuts, sides, doc_in, res_in, *refs):
    refs = list(refs)
    place_ref = refs.pop(0)
    docs = [refs.pop(0) for _ in range(n_docs)]
    owners = [refs.pop(0) for _ in range(n_docs)]
    res = [refs.pop(0) for _ in range(n_res)]
    doc_prev = [refs.pop(0) if f else None for f in doc_in]
    res_prev = [refs.pop(0) if f else None for f in res_in]
    doc_out = [refs.pop(0) for _ in range(n_docs)]
    res_out = [refs.pop(0) for _ in range(n_res)]
    work = []
    for i in range(n_docs):
        for j in range(n_res):
            rows = res[j].shape[0]
            tile = min(TILE, rows)
            work += [(i, j, t, tile) for t in range(0, rows, tile)]

    def scores(i, j, t, tile):
        return lax.dot_general(
            docs[i][...], res[j][t : t + tile, :], NT, preferred_element_type=jnp.float32
        )

    seen = set()
    doing = None
    ahead = scores(*work[0])
    for w, (i, j, t, tile) in enumerate(work):
        n = docs[i].shape[0]
        if doing != i:
            doing = i
            bias = {}
            for side in sorted(set(sides)):
                steps = place_ref[side : side + 1, :n] - owners[i][:, cuts[i]]
                steps = jnp.where(steps < 0, steps + cycle, steps)
                row = jnp.where(steps <= CYCLE_STEPS, -GAIN, OFF).astype(jnp.float32)
                bias[side] = jnp.broadcast_to(row, (LANES, n)).T
            total = jnp.zeros((n, LANES), jnp.float32)
        s = ahead
        if w + 1 < len(work):
            ahead = scores(*work[w + 1])
        for q in range(0, tile, LANES):
            k = jnp.exp2(s[:, q : q + LANES] * GAIN + bias[sides[j]])
            total = total + k
            part = jnp.sum(k, axis=0, keepdims=True)
            col = slice(t + q, t + q + LANES)
            if (j, t + q) in seen:
                part = part + res_out[j][:, col]
            elif res_prev[j] is not None:
                part = part + res_prev[j][:, col]
            seen.add((j, t + q))
            res_out[j][:, col] = part
        if w + 1 == len(work) or work[w + 1][0] != i:
            row = jnp.sum(total.T, axis=0, keepdims=True)
            if doc_prev[i] is not None:
                row = row + doc_prev[i][...]
            doc_out[i][...] = row


def held(value):
    return pltpu.with_memory_space_constraint(value, pltpu.VMEM)


def kernel_sums(cycle, place, chunks, res, sides, doc_prev, res_prev):
    docs, owners, cuts = zip(*chunks)
    doc_in = tuple(x is not None for x in doc_prev)
    res_in = tuple(x is not None for x in res_prev)
    n = sum(x.shape[0] for x in docs)
    m = sum(x.shape[0] for x in res)
    docs = [held(x) for x in docs]
    res = [held(x) for x in res]
    operands = [place, *docs, *owners, *res]
    operands += [x for x in doc_prev if x is not None]
    operands += [x for x in res_prev if x is not None]
    out = pl.pallas_call(
        functools.partial(sums_body, len(docs), len(res), cycle, cuts, tuple(sides), doc_in, res_in),
        in_specs=[VMEM] * len(operands),
        out_specs=[VMEM] * (len(docs) + len(res)),
        out_shape=[jax.ShapeDtypeStruct((1, x.shape[0]), jnp.float32) for x in (*docs, *res)],
        compiler_params=pltpu.CompilerParams(vmem_limit_bytes=24 * 2**20),
        cost_estimate=pl.CostEstimate(
            flops=2 * n * m * docs[0].shape[1], bytes_accessed=(n + m) * 1536, transcendentals=n * m
        ),
    )(*operands)
    return list(out[: len(docs)]), list(out[len(docs) :])


def line_order(count):
    return [0] + list(range(1, count, 2)) + list(reversed(range(2, count, 2)))


def dense(resident, ingest, cluster_ids):
    return dense_body(resident, ingest, cluster_ids)


def dense_body(resident, ingest, cluster_ids):
    cycle = lax.axis_size("blk")
    lines = cycle // 2
    order = line_order(lines)
    count, _ = ingest.shape
    cuts = (0, count * FIRST // 16, count)
    parts = [slice(cuts[k], cuts[k + 1]) for k in range(2)]

    def along(value, steps):
        pairs = [
            (order[k] * 2 + y, order[(k + steps) % lines] * 2 + y) for k in range(lines) for y in range(2)
        ]
        return lax.ppermute(value, "blk", pairs)

    def mate(value):
        return lax.ppermute(value, "blk", [(p, p ^ 1) for p in range(cycle)])

    def twin(value):
        return lax.ppermute(value, "rep", [(0, 1), (1, 0)])

    here = lax.axis_index("blk")
    place = jnp.stack([here, here ^ 1]).astype(jnp.int32)
    place = jnp.broadcast_to(place[:, None], (2, count))

    own = unit_rows_call(ingest, parts, parts)
    units = [own]
    owners = [(cluster_ids // CL_OWN).reshape(1, count)]
    for d in range(1, lines):
        units.append([along(units[-1][k], 1) for k in range(2)])
        owners.append(along(owners[-1], 1))
    chunks = [[(units[d][k], owners[d], parts[k]) for k in range(2)] for d in range(lines)]

    rows = resident.shape[0]
    whole = slice(0, rows)
    halves = [slice(0, rows // 2), slice(rows // 2, rows)]
    quarters = [slice(k * rows // 4, (k + 1) * rows // 4) for k in range(4)]
    r0, *r0_halves = unit_rows_call(resident, quarters, [whole, *halves])
    r2 = [mate(r0_halves[k]) for k in range(2)]
    r1 = twin(r0)
    r3 = [twin(r2[k]) for k in range(2)]
    ra = [r2[0], r3[0]]
    rb = [r2[1], r3[1]]

    def sums(docs, res, sides, doc_prev, res_prev):
        return kernel_sums(cycle, place, docs, res, sides, doc_prev, res_prev)

    d_own, a0 = sums(chunks[0], [r0], [0], [None] * 2, [None])
    d_own, a1 = sums(chunks[0], [r1], [0], d_own, [None])
    a = a0 + a1
    d1, d2 = [], []
    for k in range(2):
        d, a = sums(chunks[1][k : k + 1], [r0, r1], [0, 0], [None], a)
        d1 += d
    d, aa = sums(chunks[0] + chunks[1], ra, [1, 1], d_own + d1, [None] * 2)
    d_own, d1 = d[:2], d[2:]
    a = a + aa
    for k in range(2):
        d, a = sums(chunks[2][k : k + 1], [r0, r1, *ra], [0, 0, 1, 1], [None], a)
        d2 += d
    d, ab = sums(chunks[0] + chunks[1] + chunks[2], rb, [1, 1], d_own + d1 + d2, [None] * 2)
    d_own, d1, d2 = d[:2], d[2:4], d[4:]
    d3a, a = sums(chunks[3][:1], [r0, r1, *ra, *rb], [0, 0, 1, 1, 1, 1], [None], a + ab)
    d3b, (s0, s1, s2a, s3a, s2b, s3b) = sums(chunks[3][1:], [r0, r1, *ra, *rb], [0, 0, 1, 1, 1, 1], [None], a)
    to_twin = jnp.concatenate([s1, s3a, s3b], axis=1)
    from_twin = twin(to_twin)
    to_mate = jnp.concatenate([s2a, s2b], axis=1) + from_twin[:, rows:]
    from_mate = mate(to_mate)
    resident_density = s0 + from_twin[:, :rows] + from_mate

    ingest_density = jnp.concatenate(d_own, axis=1)
    for d, pieces in ((1, d1), (2, d2), (3, d3a + d3b)):
        pieces = jnp.concatenate(pieces, axis=1)
        ingest_density = ingest_density + along(pieces, -d)
    return (jnp.log1p(resident_density).reshape(-1), jnp.log1p(ingest_density).reshape(-1))


def shifted(value, axis, steps):
    count = lax.axis_size(axis)
    pairs = [(source, (source + steps) % count) for source in range(count)]
    return lax.ppermute(value, axis, pairs)


def unit_rows(rows):
    values = rows.astype(jnp.float32)
    squares = jnp.sum(values * values, axis=-1, keepdims=True) + epsilon
    factor = lax.rsqrt(squares)
    return (values * factor).astype(jnp.bfloat16)


def scanned_sums(visitors, occupancy, residents):
    count_rows = visitors.shape[0]
    block_rows = 512
    num_blocks = count_rows // block_rows
    visit_blocks = visitors.reshape(num_blocks, block_rows, visitors.shape[1])
    live_blocks = occupancy.astype(jnp.float32).reshape(num_blocks, block_rows)

    def tile_sums(running, pieces):
        visit_tile, live_tile = pieces
        scores = jnp.einsum("vd,rd->vr", visit_tile, residents, preferred_element_type=jnp.float32)
        kernel = jnp.exp((scores - 1.0) / temper)
        return (running + jnp.sum(kernel * live_tile[:, None], axis=0), jnp.sum(kernel, axis=1))

    resident_part, visit_parts = lax.scan(
        tile_sums, jnp.zeros((residents.shape[0],), jnp.float32), (visit_blocks, live_blocks)
    )
    return (visit_parts.reshape(count_rows), resident_part)


def cyclic(resident, ingest, cluster_ids):
    cycle_size = lax.axis_size("blk")
    slot_count = 3 * INGEST_DEV // (2 * cycle_size)
    columns = ingest.shape[1]
    owners = cluster_ids // CL_OWN
    onehot = (owners[:, None] == jnp.arange(cycle_size, dtype=jnp.int32)[None, :]).astype(jnp.int32)
    rank_within = jnp.sum((jnp.cumsum(onehot, axis=0) - onehot) * onehot, axis=1)
    targets = owners * slot_count + rank_within
    unit_ingest = unit_rows(ingest)
    outgoing = jnp.zeros((cycle_size * slot_count, columns), jnp.bfloat16).at[targets].set(unit_ingest)
    filled = (
        jnp.zeros((cycle_size * slot_count,), jnp.bfloat16)
        .at[targets]
        .set(jnp.ones((ingest.shape[0],), jnp.bfloat16))
    )
    exchange = functools.partial(lax.all_to_all, axis_name="blk", split_axis=0, concat_axis=0, tiled=True)
    arrived = exchange(outgoing.reshape(cycle_size, slot_count, columns))
    present = exchange(filled.reshape(cycle_size, slot_count))
    visitors = lax.all_gather(arrived.reshape(cycle_size * slot_count, columns), "rep", axis=0, tiled=True)
    marked = lax.all_gather(present.reshape(cycle_size * slot_count), "rep", axis=0, tiled=True)
    visit_total = jnp.zeros((visitors.shape[0],), jnp.float32)
    resident_total = jnp.zeros((resident.shape[0],), jnp.float32)
    moving = unit_rows(resident)
    for rotation in range(CYCLE_STEPS + 1):
        if rotation > 0:
            moving = shifted(moving, "blk", -1)
            resident_total = shifted(resident_total, "blk", -1)
        visit_part, resident_part = scanned_sums(visitors, marked, moving)
        visit_total = visit_total + visit_part
        resident_total = resident_total + resident_part
    resident_total = shifted(resident_total, "blk", CYCLE_STEPS)
    own_sums = lax.psum_scatter(visit_total, "rep", scatter_dimension=0, tiled=True)
    returned = exchange(own_sums.reshape(cycle_size, slot_count))
    density = returned.reshape(cycle_size * slot_count)[targets]
    return (jnp.log1p(resident_total), jnp.log1p(density))


def solution(mesh):
    spread = ("groups", "blk", "rep")
    in_specs = (P(spread, None), P(spread, None), P(spread))
    out_specs = (P(spread), P(spread))
    short = mesh.shape["blk"] == 8 and mesh.shape["rep"] == 2
    return jax.shard_map(
        dense if short else cyclic, mesh=mesh, in_specs=in_specs, out_specs=out_specs, check_vma=False
    )
```

```python
import functools

import jax
import jax.numpy as jnp
from jax import lax
from jax.experimental import pallas as pl
from jax.experimental.pallas import tpu as pltpu
from jax.sharding import PartitionSpec as P


CL_OWN = 16
CYCLE_STEPS = 4
INGEST_DEV = 512

temper = 0.2
epsilon = 1e-06


GAIN = 1.4426950408889634 / temper
OFF = -1e30
LANES = 128
NT = (((1,), (1,)), ((), ()))
VMEM = pl.BlockSpec(memory_space=pltpu.VMEM)
TILE = 512
FIRST = 8


def unit(values):
    values = values.astype(jnp.float32)
    squares = jnp.sum(values * values, axis=-1, keepdims=True) + epsilon
    return (values * lax.rsqrt(squares)).astype(jnp.bfloat16)


def unit_body(pieces, outs, x_ref, *refs):
    o_refs, raw_ref, sem = refs[: len(outs)], refs[-2], refs[-1]
    copies = [
        pltpu.make_async_copy(x_ref.at[piece], raw_ref.at[piece], sem.at[k]) for k, piece in enumerate(pieces)
    ]
    for copy in copies:
        copy.start()
    for copy, piece in zip(copies, pieces):
        copy.wait()
        rows = unit(raw_ref[piece, :])
        for o_ref, out in zip(o_refs, outs):
            if out.start <= piece.start and piece.stop <= out.stop:
                o_ref[piece.start - out.start : piece.stop - out.start, :] = rows


def unit_rows_call(rows, pieces, outs):
    columns = rows.shape[1]
    sizes = [out.stop - out.start for out in outs]
    return list(
        pl.pallas_call(
            functools.partial(unit_body, pieces, outs),
            in_specs=[pl.BlockSpec(memory_space=pltpu.HBM)],
            out_specs=[VMEM] * len(outs),
            out_shape=[pltpu.VMEM((size, columns), jnp.bfloat16) for size in sizes],
            scratch_shapes=[pltpu.VMEM(rows.shape, jnp.bfloat16), pltpu.SemaphoreType.DMA((len(pieces),))],
            compiler_params=pltpu.CompilerParams(vmem_limit_bytes=24 * 2**20),
            cost_estimate=pl.CostEstimate(
                flops=rows.size * 300, bytes_accessed=rows.size * 4, transcendentals=rows.shape[0]
            ),
        )(pltpu.with_memory_space_constraint(rows, pltpu.HBM))
    )


def sums_body(n_docs, n_res, cycle, cuts, sides, doc_in, res_in, *refs):
    refs = list(refs)
    place_ref = refs.pop(0)
    docs = [refs.pop(0) for _ in range(n_docs)]
    owners = [refs.pop(0) for _ in range(n_docs)]
    res = [refs.pop(0) for _ in range(n_res)]
    doc_prev = [refs.pop(0) if f else None for f in doc_in]
    res_prev = [refs.pop(0) if f else None for f in res_in]
    doc_out = [refs.pop(0) for _ in range(n_docs)]
    res_out = [refs.pop(0) for _ in range(n_res)]
    work = []
    for i in range(n_docs):
        for j in range(n_res):
            rows = res[j].shape[0]
            tile = min(TILE, rows)
            work += [(i, j, t, tile) for t in range(0, rows, tile)]

    def scores(i, j, t, tile):
        return lax.dot_general(
            docs[i][...], res[j][t : t + tile, :], NT, preferred_element_type=jnp.float32
        )

    seen = set()
    doing = None
    ahead = scores(*work[0])
    for w, (i, j, t, tile) in enumerate(work):
        n = docs[i].shape[0]
        if doing != i:
            doing = i
            bias = {}
            for side in sorted(set(sides)):
                steps = place_ref[side : side + 1, :n] - owners[i][:, cuts[i]]
                steps = jnp.where(steps < 0, steps + cycle, steps)
                row = jnp.where(steps <= CYCLE_STEPS, -GAIN, OFF).astype(jnp.float32)
                bias[side] = jnp.broadcast_to(row, (LANES, n)).T
            total = jnp.zeros((n, LANES), jnp.float32)
        s = ahead
        if w + 1 < len(work):
            ahead = scores(*work[w + 1])
        for q in range(0, tile, LANES):
            k = jnp.exp2(s[:, q : q + LANES] * GAIN + bias[sides[j]])
            total = total + k
            part = jnp.sum(k, axis=0, keepdims=True)
            col = slice(t + q, t + q + LANES)
            if (j, t + q) in seen:
                part = part + res_out[j][:, col]
            elif res_prev[j] is not None:
                part = part + res_prev[j][:, col]
            seen.add((j, t + q))
            res_out[j][:, col] = part
        if w + 1 == len(work) or work[w + 1][0] != i:
            row = jnp.sum(total.T, axis=0, keepdims=True)
            if doc_prev[i] is not None:
                row = row + doc_prev[i][...]
            doc_out[i][...] = row


def held(value):
    return pltpu.with_memory_space_constraint(value, pltpu.VMEM)


def kernel_sums(cycle, place, chunks, res, sides, doc_prev, res_prev):
    docs, owners, cuts = zip(*chunks)
    doc_in = tuple(x is not None for x in doc_prev)
    res_in = tuple(x is not None for x in res_prev)
    n = sum(x.shape[0] for x in docs)
    m = sum(x.shape[0] for x in res)
    docs = [held(x) for x in docs]
    res = [held(x) for x in res]
    operands = [place, *docs, *owners, *res]
    operands += [x for x in doc_prev if x is not None]
    operands += [x for x in res_prev if x is not None]
    out = pl.pallas_call(
        functools.partial(sums_body, len(docs), len(res), cycle, cuts, tuple(sides), doc_in, res_in),
        in_specs=[VMEM] * len(operands),
        out_specs=[VMEM] * (len(docs) + len(res)),
        out_shape=[jax.ShapeDtypeStruct((1, x.shape[0]), jnp.float32) for x in (*docs, *res)],
        compiler_params=pltpu.CompilerParams(vmem_limit_bytes=24 * 2**20),
        cost_estimate=pl.CostEstimate(
            flops=2 * n * m * docs[0].shape[1], bytes_accessed=(n + m) * 1536, transcendentals=n * m
        ),
    )(*operands)
    return list(out[: len(docs)]), list(out[len(docs) :])


def scores_body(n_res, n_doc, *refs):
    terms, (res_hbm, doc_hbm, res_ref, doc_ref, sem) = refs[:-5], refs[-5:]
    res_rows = res_ref.shape[1]
    total = terms[0][:, :res_rows]
    for term in terms[1:n_res]:
        total = total + term[:, :res_rows]
    res_ref[...] = jnp.log1p(total)
    first = pltpu.make_async_copy(res_ref, res_hbm, sem.at[0])
    first.start()
    total = jnp.concatenate([term[...] for term in terms[n_res : n_res + n_doc]], axis=1)
    for term in terms[n_res + n_doc :]:
        total = total + term[...]
    doc_ref[...] = jnp.log1p(total)
    second = pltpu.make_async_copy(doc_ref, doc_hbm, sem.at[1])
    second.start()
    first.wait()
    second.wait()


def scores_call(rows, count, res_terms, own_terms, doc_terms):
    shapes = [(1, rows), (1, count)]
    return pl.pallas_call(
        functools.partial(scores_body, len(res_terms), len(own_terms)),
        in_specs=[VMEM] * (len(res_terms) + len(own_terms) + len(doc_terms)),
        out_specs=[pl.BlockSpec(memory_space=pltpu.HBM)] * 2,
        out_shape=[jax.ShapeDtypeStruct(shape, jnp.float32) for shape in shapes],
        scratch_shapes=[pltpu.VMEM(shape, jnp.float32) for shape in shapes] + [pltpu.SemaphoreType.DMA((2,))],
        name="scores",
        compiler_params=pltpu.CompilerParams(vmem_limit_bytes=8 * 2**20),
    )(*res_terms, *own_terms, *doc_terms)


def line_order(count):
    return [0] + list(range(1, count, 2)) + list(reversed(range(2, count, 2)))


def dense(resident, ingest, cluster_ids):
    return dense_body(resident, ingest, cluster_ids)


def dense_body(resident, ingest, cluster_ids):
    cycle = lax.axis_size("blk")
    lines = cycle // 2
    order = line_order(lines)
    count, _ = ingest.shape
    cuts = (0, count * FIRST // 16, count)
    parts = [slice(cuts[k], cuts[k + 1]) for k in range(2)]

    def along(value, steps):
        pairs = [
            (order[k] * 2 + y, order[(k + steps) % lines] * 2 + y) for k in range(lines) for y in range(2)
        ]
        return lax.ppermute(value, "blk", pairs)

    def mate(value):
        return lax.ppermute(value, "blk", [(p, p ^ 1) for p in range(cycle)])

    def twin(value):
        return lax.ppermute(value, "rep", [(0, 1), (1, 0)])

    here = lax.axis_index("blk")
    place = jnp.stack([here, here ^ 1]).astype(jnp.int32)
    place = jnp.broadcast_to(place[:, None], (2, count))

    own = [unit_rows_call(ingest, [parts[k]], [parts[k]])[0] for k in range(2)]
    units = [own]
    owners = [(cluster_ids // CL_OWN).reshape(1, count)]
    for d in range(1, lines):
        units.append([along(units[-1][k], 1) for k in range(2)])
        owners.append(along(owners[-1], 1))
    chunks = [[(units[d][k], owners[d], parts[k]) for k in range(2)] for d in range(lines)]

    rows = resident.shape[0]
    whole = slice(0, rows)
    halves = [slice(0, rows // 2), slice(rows // 2, rows)]
    quarters = [slice(k * rows // 4, (k + 1) * rows // 4) for k in range(4)]
    r0, *r0_halves = unit_rows_call(resident, quarters, [whole, *halves])
    r2 = [mate(r0_halves[k]) for k in range(2)]
    r1 = twin(r0)
    r3 = [twin(r2[k]) for k in range(2)]
    ra = [r2[0], r3[0]]
    rb = [r2[1], r3[1]]

    def sums(docs, res, sides, doc_prev, res_prev):
        return kernel_sums(cycle, place, docs, res, sides, doc_prev, res_prev)

    d_own, a0 = sums(chunks[0], [r0], [0], [None] * 2, [None])
    d_own, a1 = sums(chunks[0], [r1], [0], d_own, [None])
    a = a0 + a1
    d1, d2 = [], []
    for k in range(2):
        d, a = sums(chunks[1][k : k + 1], [r0, r1], [0, 0], [None], a)
        d1 += d
    d, aa = sums(chunks[0] + chunks[1], ra, [1, 1], d_own + d1, [None] * 2)
    d_own, d1 = d[:2], d[2:]
    a = a + aa
    for k in range(2):
        d, a = sums(chunks[2][k : k + 1], [r0, r1, *ra], [0, 0, 1, 1], [None], a)
        d2 += d
    d, ab = sums(chunks[0] + chunks[1] + chunks[2], rb, [1, 1], d_own + d1 + d2, [None] * 2)
    d_own, d1, d2 = d[:2], d[2:4], d[4:]
    d3a, a = sums(chunks[3][:1], [r0, r1, *ra, *rb], [0, 0, 1, 1, 1, 1], [None], a + ab)
    d3b, (s0, s1, s2a, s3a, s2b, s3b) = sums(chunks[3][1:], [r0, r1, *ra, *rb], [0, 0, 1, 1, 1, 1], [None], a)
    to_twin = jnp.concatenate([s1, s3a, s3b], axis=1)
    from_twin = twin(to_twin)
    to_mate = jnp.concatenate([s2a, s2b], axis=1) + from_twin[:, rows:]
    from_mate = mate(to_mate)
    backs = []
    for d, pieces in ((1, d1), (2, d2), (3, d3a + d3b)):
        pieces = jnp.concatenate(pieces, axis=1)
        backs.append(along(pieces, -d))
    res_scores, doc_scores = scores_call(rows, count, [s0, from_twin, from_mate], d_own, backs)
    return res_scores.reshape(-1), doc_scores.reshape(-1)


def shifted(value, axis, steps):
    count = lax.axis_size(axis)
    pairs = [(source, (source + steps) % count) for source in range(count)]
    return lax.ppermute(value, axis, pairs)


def unit_rows(rows):
    values = rows.astype(jnp.float32)
    squares = jnp.sum(values * values, axis=-1, keepdims=True) + epsilon
    factor = lax.rsqrt(squares)
    return (values * factor).astype(jnp.bfloat16)


def scanned_sums(visitors, occupancy, residents):
    count_rows = visitors.shape[0]
    block_rows = 512
    num_blocks = count_rows // block_rows
    visit_blocks = visitors.reshape(num_blocks, block_rows, visitors.shape[1])
    live_blocks = occupancy.astype(jnp.float32).reshape(num_blocks, block_rows)

    def tile_sums(running, pieces):
        visit_tile, live_tile = pieces
        scores = jnp.einsum("vd,rd->vr", visit_tile, residents, preferred_element_type=jnp.float32)
        kernel = jnp.exp((scores - 1.0) / temper)
        return (running + jnp.sum(kernel * live_tile[:, None], axis=0), jnp.sum(kernel, axis=1))

    resident_part, visit_parts = lax.scan(
        tile_sums, jnp.zeros((residents.shape[0],), jnp.float32), (visit_blocks, live_blocks)
    )
    return (visit_parts.reshape(count_rows), resident_part)


def cyclic(resident, ingest, cluster_ids):
    cycle_size = lax.axis_size("blk")
    slot_count = 3 * INGEST_DEV // (2 * cycle_size)
    columns = ingest.shape[1]
    owners = cluster_ids // CL_OWN
    onehot = (owners[:, None] == jnp.arange(cycle_size, dtype=jnp.int32)[None, :]).astype(jnp.int32)
    rank_within = jnp.sum((jnp.cumsum(onehot, axis=0) - onehot) * onehot, axis=1)
    targets = owners * slot_count + rank_within
    unit_ingest = unit_rows(ingest)
    outgoing = jnp.zeros((cycle_size * slot_count, columns), jnp.bfloat16).at[targets].set(unit_ingest)
    filled = (
        jnp.zeros((cycle_size * slot_count,), jnp.bfloat16)
        .at[targets]
        .set(jnp.ones((ingest.shape[0],), jnp.bfloat16))
    )
    exchange = functools.partial(lax.all_to_all, axis_name="blk", split_axis=0, concat_axis=0, tiled=True)
    arrived = exchange(outgoing.reshape(cycle_size, slot_count, columns))
    present = exchange(filled.reshape(cycle_size, slot_count))
    visitors = lax.all_gather(arrived.reshape(cycle_size * slot_count, columns), "rep", axis=0, tiled=True)
    marked = lax.all_gather(present.reshape(cycle_size * slot_count), "rep", axis=0, tiled=True)
    visit_total = jnp.zeros((visitors.shape[0],), jnp.float32)
    resident_total = jnp.zeros((resident.shape[0],), jnp.float32)
    moving = unit_rows(resident)
    for rotation in range(CYCLE_STEPS + 1):
        if rotation > 0:
            moving = shifted(moving, "blk", -1)
            resident_total = shifted(resident_total, "blk", -1)
        visit_part, resident_part = scanned_sums(visitors, marked, moving)
        visit_total = visit_total + visit_part
        resident_total = resident_total + resident_part
    resident_total = shifted(resident_total, "blk", CYCLE_STEPS)
    own_sums = lax.psum_scatter(visit_total, "rep", scatter_dimension=0, tiled=True)
    returned = exchange(own_sums.reshape(cycle_size, slot_count))
    density = returned.reshape(cycle_size * slot_count)[targets]
    return (jnp.log1p(resident_total), jnp.log1p(density))


def solution(mesh):
    spread = ("groups", "blk", "rep")
    in_specs = (P(spread, None), P(spread, None), P(spread))
    out_specs = (P(spread), P(spread))
    short = mesh.shape["blk"] == 8 and mesh.shape["rep"] == 2
    return jax.shard_map(
        dense if short else cyclic, mesh=mesh, in_specs=in_specs, out_specs=out_specs, check_vma=False
    )
```
